32 devices in a mesh: data: 4 (over y, z), tp: 8 (over x, core).
Axes of the slice: x: 4, y: 2, z: 2, core: 2. Of those that a mesh axis runs over, the one named last changes fastest.
The devices are a block of a 4x4x8 slice.
Arguments:
- hidden_acts: bfloat16 [16384, 14336], P('data', 'tp'), parts along dimension 0
- w_down: bfloat16 [14336, 3584], P('tp')
- w_next: bfloat16 [3584, 8192], P(None, 'tp')
Outputs:
- output: bfloat16 [16384, 8192], P('data', 'tp'), parts along dimension 0
There are 4 independent parts. The reference program is written for one: setup_inputs(seed, part) draws one part's arguments, and reference() takes and returns one part's arrays. A program takes and returns all parts, laid end to end along the dimension named above; an argument that names none is the same for every part.
All inputs are finite; a program needn't handle non-finite values.
Results may differ from the reference program's by a relative error of at most 0.00114.
Values are sent between devices in bfloat16 or wider.
A program may use at most 768 MiB of HBM per device.

```python
import jax
import jax.numpy as jnp

TOKENS = 4096
FFN_DIM = 14336
HIDDEN = 3584
QKV_DIM = 8192


def setup_inputs(seed: int = 0, part: int = 0) -> dict:
    root_key = jax.random.key(seed)
    key_x = jax.random.fold_in(jax.random.fold_in(root_key, 1), part)
    key_w = jax.random.fold_in(root_key, 2)
    key_v = jax.random.fold_in(root_key, 3)
    hidden_acts = jax.random.normal(key_x, (TOKENS, FFN_DIM), jnp.float32)
    w_down = jax.random.normal(key_w, (FFN_DIM, HIDDEN), jnp.float32) * FFN_DIM ** -0.5
    w_next = jax.random.normal(key_v, (HIDDEN, QKV_DIM), jnp.float32) * HIDDEN ** -0.5
    return {"hidden_acts": hidden_acts.astype(jnp.bfloat16), "w_down": w_down.astype(jnp.bfloat16), "w_next": w_next.astype(jnp.bfloat16)}


def reference(hidden_acts, w_down, w_next):
    mixed = jnp.dot(hidden_acts, w_down, preferred_element_type=jnp.float32).astype(jnp.bfloat16)
    return jnp.dot(mixed, w_next, preferred_element_type=jnp.float32).astype(jnp.bfloat16)
```

```python
import functools

import jax
import jax.numpy as jnp
from jax import lax
from jax.experimental import pallas as pl
from jax.experimental.pallas import tpu as pltpu
from jax.sharding import PartitionSpec as P

MESH = pl.DeviceIdType.MESH
UNIT = 32
P_SLOTS, D_SLOTS, HOP_SLOTS, ROOT_SLOTS, Y_SLOTS = 3, 2, 4, 4, 6
PLUS, MINUS = 0, 1


def kernel(ring, rounds, x_hbm, w_hbm, v_hbm, u_hbm, w_vm, v_vm, x_vm, part, pair, hop, root, y_vm, u_vm,
           w_sem, v_sem, x_sem, u_sem, pair_send, pair_recv, hop_send, hop_recv, dir_send, dir_recv, fwd_send, fwd_recv,
           ag_send, ag_recv, agf_send, agf_recv, yp_send, yp_recv):
    width = w_hbm.shape[1]
    half = width // 2
    rows = x_vm.shape[1]
    me = lax.axis_index("tp")
    chip, core = me // 2, lax.rem(me, 2)
    right, left, far = lax.rem(chip + 1, ring), lax.rem(chip + ring - 1, ring), lax.rem(chip + 2, ring)
    partner = {"tp": chip * 2 + 1 - core}
    to = ({"tp": right * 2 + core}, {"tp": left * 2 + core})
    mine, theirs = core * ring, (1 - core) * ring
    cols = (pl.ds(0, half), pl.ds(half, half))

    def remote(src, dst, send, recv, where):
        return pltpu.make_async_remote_copy(src_ref=src, dst_ref=dst, send_sem=send, recv_sem=recv, device_id=where, device_id_type=MESH)

    def load_x(k):
        return pltpu.make_async_copy(x_hbm.at[pl.ds(k * rows, rows)], x_vm.at[lax.rem(k, 2)], x_sem.at[lax.rem(k, 2)])

    def load_w(h):
        return pltpu.make_async_copy(w_hbm.at[:, cols[h]], w_vm.at[:, cols[h]], w_sem.at[h])

    def load_v():
        return pltpu.make_async_copy(v_hbm, v_vm, v_sem)

    def store_u(k):
        return pltpu.make_async_copy(u_vm.at[lax.rem(k, 2)], u_hbm.at[pl.ds(k * rows, rows)], u_sem.at[lax.rem(k, 2)])

    def pair_copy(k, h):
        s, d = lax.rem(k, P_SLOTS), lax.rem(k, D_SLOTS)
        return remote(part.at[s, pl.ds(theirs, ring), :, cols[h]], pair.at[d, :, :, cols[h]], pair_send.at[s, h], pair_recv.at[d, h], partner)

    def hop_copy(k, d):
        s, t = lax.rem(k, P_SLOTS), lax.rem(k, HOP_SLOTS)
        return remote(part.at[s, mine + far, :, cols[d]], hop.at[t, d], hop_send.at[s, d], hop_recv.at[t, d], to[d])

    def dir_copy(k, d):
        s, t = lax.rem(k, P_SLOTS), lax.rem(k, ROOT_SLOTS)
        unit = right if d == PLUS else left
        return remote(part.at[s, mine + unit, :, cols[1 - d]], root.at[t, d, 1 - d], dir_send.at[s, d], dir_recv.at[t, d], to[d])

    def fwd_copy(k, d):
        s, t = lax.rem(k, P_SLOTS), lax.rem(k, ROOT_SLOTS)
        unit = right if d == PLUS else left
        return remote(part.at[s, mine + unit, :, cols[d]], root.at[t, d, d], fwd_send.at[s, d], fwd_recv.at[t, d], to[d])

    def ag_copy(k, d):
        t = lax.rem(k, Y_SLOTS)
        ref = y_vm.at[t, mine + chip]
        return remote(ref, ref, ag_send.at[t, d], ag_recv.at[t, d], to[d])

    def agf_copy(k, d):
        t = lax.rem(k, Y_SLOTS)
        unit = left if d == PLUS else right
        ref = y_vm.at[t, mine + unit, :, cols[d]]
        return remote(ref, ref, agf_send.at[t, d], agf_recv.at[t, d], to[d])

    def yp_copy(k, unit):
        t = lax.rem(k, Y_SLOTS)
        ref = y_vm.at[t, mine + unit]
        return remote(ref, ref, yp_send.at[t, unit], yp_recv.at[t, unit], partner)

    load_x(0).start()
    load_w(0).start()
    load_w(1).start()
    load_v().start()

    barrier = pltpu.get_barrier_semaphore()
    for other in (partner, *to):
        pl.semaphore_signal(barrier, inc=1, device_id=other, device_id_type=MESH)
    pl.semaphore_wait(barrier, 3)

    def wait_part_sends(k):
        for h in (0, 1):
            pair_copy(k, h).wait_send()
            hop_copy(k, h).wait_send()
            dir_copy(k, h).wait_send()
            fwd_copy(k, h).wait_send()

    def product(k):
        load_x(k).wait()

        @pl.when(k + 1 < rounds)
        def _():
            load_x(k + 1).start()

        @pl.when(k >= P_SLOTS)
        def _():
            wait_part_sends(k - P_SLOTS)

        s = lax.rem(k, P_SLOTS)
        for h in (0, 1):
            @pl.when(k == 0)
            def _():
                load_w(h).wait()

            acc = jnp.dot(x_vm[lax.rem(k, 2)], w_vm[:, cols[h]], preferred_element_type=jnp.float32)
            part[s, :, :, cols[h]] = acc.reshape(2 * ring, UNIT, half)
            pair_copy(k, h).start()

    def pair_sum(k):
        s, d = lax.rem(k, P_SLOTS), lax.rem(k, D_SLOTS)

        def add(unit, h):
            part[s, mine + unit, :, cols[h]] += pair[d, unit, :, cols[h]]

        pair_copy(k, 0).wait_recv()
        add(far, 0)
        hop_copy(k, PLUS).start()
        pair_copy(k, 1).wait_recv()
        add(far, 1)
        hop_copy(k, MINUS).start()
        add(right, 1)
        dir_copy(k, PLUS).start()
        add(left, 0)
        dir_copy(k, MINUS).start()
        add(right, 0)
        add(left, 1)
        add(chip, 0)
        add(chip, 1)

    def relay(k):
        s, t = lax.rem(k, P_SLOTS), lax.rem(k, HOP_SLOTS)
        for d in (PLUS, MINUS):
            unit = right if d == PLUS else left
            hop_copy(k, d).wait_recv()
            part[s, mine + unit, :, cols[d]] += hop[t, d]
            fwd_copy(k, d).start()

    def finish(k):
        s, t, y = lax.rem(k, P_SLOTS), lax.rem(k, ROOT_SLOTS), lax.rem(k, Y_SLOTS)
        for d in (PLUS, MINUS):
            dir_copy(k, d).wait_recv()
            fwd_copy(k, d).wait_recv()
        for h in (0, 1):
            total = part[s, mine + chip, :, cols[h]] + root[t, PLUS, h] + root[t, MINUS, h]
            y_vm[y, mine + chip, :, cols[h]] = total.astype(jnp.bfloat16)
        for d in (PLUS, MINUS):
            ag_copy(k, d).start()
        yp_copy(k, chip).start()

    def spread(k):
        for d in (PLUS, MINUS):
            ag_copy(k, d).wait_recv()
            agf_copy(k, d).start()
        yp_copy(k, left).start()
        yp_copy(k, right).start()

    def share(k):
        for d in (PLUS, MINUS):
            agf_copy(k, d).wait_recv()
        yp_copy(k, far).start()

    def project(k):
        y = lax.rem(k, Y_SLOTS)
        for unit in range(ring):
            yp_copy(k, unit).wait_recv()
        for d in (PLUS, MINUS):
            ag_copy(k, d).wait_send()
            agf_copy(k, d).wait_send()
        for unit in range(ring):
            yp_copy(k, unit).wait_send()

        @pl.when(k == 0)
        def _():
            load_v().wait()

        @pl.when(k >= 2)
        def _():
            store_u(k - 2).wait()

        full = y_vm[y].reshape(rows, width)
        u_vm[lax.rem(k, 2)] = jnp.dot(full, v_vm[...], preferred_element_type=jnp.float32).astype(jnp.bfloat16)
        store_u(k).start()

    def step(i, carry):
        for stage, lag in ((product, 0), (project, 5), (pair_sum, 0), (relay, 1), (finish, 2), (spread, 3), (share, 4)):
            k = i - lag

            @pl.when(jnp.logical_and(k >= 0, k < rounds))
            def _():
                stage(k)

        return carry

    lax.fori_loop(0, rounds + 5, step, 0)
    for k in range(rounds - P_SLOTS, rounds):
        wait_part_sends(k)
    for k in range(rounds - 2, rounds):
        store_u(k).wait()


def solution(mesh):
    ring = mesh.shape["tp"] // 2

    def local_step(x, w, v):
        tokens, depth = x.shape
        width, out = v.shape
        rows = 2 * ring * UNIT
        rounds = tokens // rows
        half = width // 2
        dma = pltpu.SemaphoreType.DMA
        f32, bf16 = jnp.float32, jnp.bfloat16
        any_spec = pl.BlockSpec(memory_space=pl.ANY)
        return pl.pallas_call(
            functools.partial(kernel, ring, rounds),
            out_shape=jax.ShapeDtypeStruct((tokens, out), bf16),
            in_specs=[any_spec] * 3,
            out_specs=any_spec,
            scratch_shapes=[
                pltpu.VMEM((depth, width), bf16),
                pltpu.VMEM((width, out), bf16),
                pltpu.VMEM((2, rows, depth), bf16),
                pltpu.VMEM((P_SLOTS, 2 * ring, UNIT, width), f32),
                pltpu.VMEM((D_SLOTS, ring, UNIT, width), f32),
                pltpu.VMEM((HOP_SLOTS, 2, UNIT, half), f32),
                pltpu.VMEM((ROOT_SLOTS, 2, 2, UNIT, half), f32),
                pltpu.VMEM((Y_SLOTS, 2 * ring, UNIT, width), bf16),
                pltpu.VMEM((2, rows, out), bf16),
                dma((2,)), dma, dma((2,)), dma((2,)),
                dma((P_SLOTS, 2)), dma((D_SLOTS, 2)),
                dma((P_SLOTS, 2)), dma((HOP_SLOTS, 2)),
                dma((P_SLOTS, 2)), dma((ROOT_SLOTS, 2)),
                dma((P_SLOTS, 2)), dma((ROOT_SLOTS, 2)),
                dma((Y_SLOTS, 2)), dma((Y_SLOTS, 2)),
                dma((Y_SLOTS, 2)), dma((Y_SLOTS, 2)),
                dma((Y_SLOTS, ring)), dma((Y_SLOTS, ring)),
            ],
            compiler_params=pltpu.CompilerParams(collective_id=0, has_side_effects=True, vmem_limit_bytes=67_043_328),
            cost_estimate=pl.CostEstimate(flops=2 * tokens * (depth * width + width * out), bytes_accessed=2 * (tokens * depth + depth * width + width * out + tokens * out), transcendentals=0),
        )(x, w, v)

    return jax.shard_map(local_step, mesh=mesh, in_specs=(P("data", "tp"), P("tp", None), P(None, "tp")), out_specs=P("data", "tp"), check_vma=False)
```

```python
import functools

import jax
import jax.numpy as jnp
from jax import lax
from jax.experimental import pallas as pl
from jax.experimental.pallas import tpu as pltpu
from jax.sharding import PartitionSpec as P

MESH = pl.DeviceIdType.MESH
UNIT = 16
TAIL = 2
P_SLOTS, D_SLOTS, HOP_SLOTS, ROOT_SLOTS, Y_SLOTS, G_SLOTS = 3, 2, 4, 4, 6, 4
PLUS, MINUS = 0, 1
WIDE, LAG, AHEAD = 512, 2, 3


def first_blocks(half):
    starts = [0, *range(half % WIDE, half, WIDE)] if half % WIDE else list(range(0, half, WIDE))
    return [(side, c, d - c) for c, d in zip(starts, starts[1:] + [half]) for side in (PLUS, MINUS)]


def reduce_and_project(ring, rounds, x_hbm, w_hbm, v_hbm, u_vm, v_vm, y_last, w_vm, x_vm, part, pair, hop, root, y_vm,
                       w_sem, v_sem, x_sem, part_send, pair_recv, first_pair, first_hop, hop_recv, root_recv,
                       y_send, ag_recv, agf_recv, yp_recv):
    width = w_hbm.shape[1]
    half = width // 2
    rows = x_vm.shape[1]
    me = lax.axis_index("tp")
    chip, core = me // 2, lax.rem(me, 2)
    right, left, far = lax.rem(chip + 1, ring), lax.rem(chip + ring - 1, ring), lax.rem(chip + 2, ring)
    partner = {"tp": chip * 2 + 1 - core}
    to = ({"tp": right * 2 + core}, {"tp": left * 2 + core})
    next_unit = (right, left)
    mine, theirs = core * ring, (1 - core) * ring
    cols = (pl.ds(0, half), pl.ds(half, half))
    blocks = first_blocks(half)

    def remote(src, dst, send, recv, where):
        return pltpu.make_async_remote_copy(src_ref=src, dst_ref=dst, send_sem=send, recv_sem=recv, device_id=where, device_id_type=MESH)

    def await_bytes(ref, sem):
        pltpu.make_async_copy(ref, ref, sem).wait()

    def fine(b):
        side, start, size = blocks[b]
        return pl.ds(side * half + start, size)

    def load_x(k):
        return pltpu.make_async_copy(x_hbm.at[pl.ds(k * rows, rows)], x_vm.at[lax.rem(k, 2)], x_sem.at[lax.rem(k, 2)])

    def load_w(b):
        return pltpu.make_async_copy(w_hbm.at[:, fine(b)], w_vm.at[:, fine(b)], w_sem.at[b])

    def load_v():
        return pltpu.make_async_copy(v_hbm, v_vm, v_sem)

    def pair_copy(k, h):
        s, d = lax.rem(k, P_SLOTS), lax.rem(k, D_SLOTS)
        return remote(part.at[s, pl.ds(theirs, ring), :, cols[h]], pair.at[d, :, :, cols[h]], part_send.at[s], pair_recv.at[d, h], partner)

    def hop_copy(k, d):
        s, t = lax.rem(k, P_SLOTS), lax.rem(k, HOP_SLOTS)
        return remote(part.at[s, mine + far, :, cols[d]], hop.at[t, d], part_send.at[s], hop_recv.at[t, d], to[d])

    def to_root(k, d, h):
        s, t = lax.rem(k, P_SLOTS), lax.rem(k, ROOT_SLOTS)
        return remote(part.at[s, mine + next_unit[d], :, cols[h]], root.at[t, d, h], part_send.at[s], root_recv.at[t], to[d])

    def ag_copy(k, d, h):
        t, g = lax.rem(k, Y_SLOTS), lax.rem(k, G_SLOTS)
        ref = y_vm.at[t, mine + chip, :, cols[h]]
        return remote(ref, ref, y_send.at[t], ag_recv.at[g, d, h], to[d])

    def agf_copy(k, d):
        t, g = lax.rem(k, Y_SLOTS), lax.rem(k, G_SLOTS)
        ref = y_vm.at[t, mine + next_unit[1 - d], :, cols[d]]
        return remote(ref, ref, y_send.at[t], agf_recv.at[g], to[d])

    def yp_copy(k, unit):
        t = lax.rem(k, Y_SLOTS)
        ref = y_vm.at[t, mine + unit]
        return remote(ref, ref, y_send.at[t], yp_recv.at[t], partner)

    def wait_part_sends(k):
        s = lax.rem(k, P_SLOTS)
        await_bytes(part.at[s, pl.ds(0, ring + 3)], part_send.at[s])

    def product_half(k, h):
        s = lax.rem(k, P_SLOTS)
        acc = jnp.dot(x_vm[lax.rem(k, 2)], w_vm[:, cols[h]], preferred_element_type=jnp.float32)
        part[s, :, :, cols[h]] = acc.reshape(2 * ring, UNIT, half)
        pair_copy(k, h).start()

    def product(k):
        load_x(k).wait()

        @pl.when(k + 1 < rounds)
        def _():
            load_x(k + 1).start()

        @pl.when(k >= P_SLOTS)
        def _():
            wait_part_sends(k - P_SLOTS)

        product_half(k, 0)
        product_half(k, 1)

    def add_pair(k, unit, h):
        s, d = lax.rem(k, P_SLOTS), lax.rem(k, D_SLOTS)
        part[s, mine + unit, :, cols[h]] += pair[d, unit, :, cols[h]]

    def pair_far(k, h):
        pair_copy(k, h).wait_recv()
        add_pair(k, far, h)
        hop_copy(k, h).start()

    def pair_rest(k):
        for d in (PLUS, MINUS):
            add_pair(k, next_unit[d], 1 - d)
            to_root(k, d, 1 - d).start()
        for d in (PLUS, MINUS):
            add_pair(k, next_unit[d], d)
        for h in (0, 1):
            add_pair(k, chip, h)

    def pair_sum(k):
        pair_far(k, 0)
        pair_far(k, 1)
        pair_rest(k)

    def relay(k):
        s, t = lax.rem(k, P_SLOTS), lax.rem(k, HOP_SLOTS)
        for d in (PLUS, MINUS):
            hop_copy(k, d).wait_recv()
            part[s, mine + next_unit[d], :, cols[d]] += hop[t, d]
            to_root(k, d, d).start()

    def finish(k):
        s, t, y = lax.rem(k, P_SLOTS), lax.rem(k, ROOT_SLOTS), lax.rem(k, Y_SLOTS)
        await_bytes(root.at[t], root_recv.at[t])
        for h in (0, 1):
            total = part[s, mine + chip, :, cols[h]] + root[t, PLUS, h] + root[t, MINUS, h]
            y_vm[y, mine + chip, :, cols[h]] = total.astype(jnp.bfloat16)
        for d in (PLUS, MINUS):
            ag_copy(k, d, d).start()
        for d in (PLUS, MINUS):
            ag_copy(k, d, 1 - d).start()
        yp_copy(k, chip).start()

    def spread(k):
        for d in (PLUS, MINUS):
            ag_copy(k, d, d).wait_recv()
            agf_copy(k, d).start()
        for d in (PLUS, MINUS):
            ag_copy(k, d, 1 - d).wait_recv()
            yp_copy(k, next_unit[1 - d]).start()

    def share(k):
        t, g = lax.rem(k, Y_SLOTS), lax.rem(k, G_SLOTS)
        await_bytes(y_vm.at[t, mine + far], agf_recv.at[g])
        yp_copy(k, far).start()

    def project(k):
        y = lax.rem(k, Y_SLOTS)
        await_bytes(y_vm.at[y, pl.ds(0, ring)], yp_recv.at[y])
        await_bytes(y_vm.at[y, pl.ds(0, ring + 3)], y_send.at[y])

        @pl.when(k == 0)
        def _():
            load_v().wait()

        @pl.when(k < rounds - TAIL)
        def _():
            full = y_vm[y].reshape(rows, width)
            u_vm[pl.ds(pl.multiple_of(k * rows, rows), rows)] = jnp.dot(full, v_vm[...], preferred_element_type=jnp.float32).astype(jnp.bfloat16)

        for n in range(TAIL):
            @pl.when(k == rounds - TAIL + n)
            def _():
                y_last[pl.ds(n * rows, rows)] = y_vm[y].reshape(rows, width)

    def first_rounds():
        def pair_fine(b):
            return remote(part.at[0, pl.ds(theirs, ring), :, fine(b)], pair.at[0, :, :, fine(b)], part_send.at[0], first_pair.at[b], partner)

        def make(b):
            load_w(b).wait()
            if b + AHEAD < len(blocks):
                load_w(b + AHEAD).start()
            acc = jnp.dot(x_vm[0], w_vm[:, fine(b)], preferred_element_type=jnp.float32)
            part[0, :, :, fine(b)] = acc.reshape(2 * ring, UNIT, acc.shape[1])
            if b == 0:
                pl.semaphore_wait(barrier, 3)
            pair_fine(b).start()

        def send(b):
            d, start, size = blocks[b]
            within = pl.ds(start, size)
            pair_fine(b).wait_recv()
            part[0, pl.ds(mine, ring), :, fine(b)] += pair[0, :, :, fine(b)]
            remote(part.at[0, mine + far, :, fine(b)], hop.at[0, d, :, within], part_send.at[0], first_hop.at[b], to[d]).start()
            e = 1 - d
            remote(part.at[0, mine + next_unit[e], :, fine(b)], root.at[0, e, d, :, within], part_send.at[0], root_recv.at[0], to[e]).start()

        def pass_on(*which):
            for b in which:
                d, start, size = blocks[b]
                within = pl.ds(start, size)
                await_bytes(hop.at[0, d, :, within], first_hop.at[b])
                part[0, mine + next_unit[d], :, fine(b)] += hop[0, d, :, within]
                remote(part.at[0, mine + next_unit[d], :, fine(b)], root.at[0, d, d, :, within], part_send.at[0], root_recv.at[0], to[d]).start()

        count = len(blocks)
        load_x(0).wait()
        load_x(1).start()
        for b in range(count + LAG):
            if b < count:
                make(b)
            if b >= LAG:
                send(b - LAG)
        pass_on(*range(count - 5))
        load_x(1).wait()
        load_x(2).start()
        product_half(1, 0)
        pass_on(*range(count - 5, count - 3))
        product_half(1, 1)
        pass_on(*range(count - 3, count - 1))
        pair_far(1, 0)
        pass_on(count - 1)
        pair_far(1, 1)
        pair_rest(1)
        load_v().start()

    load_x(0).start()
    for b in range(AHEAD):
        load_w(b).start()
    barrier = pltpu.get_barrier_semaphore()
    for other in (partner, *to):
        pl.semaphore_signal(barrier, inc=1, device_id=other, device_id_type=MESH)
    first_rounds()

    def step(i, carry):
        for stage, lag in ((product, 0), (pair_sum, 0), (relay, 1), (finish, 2), (spread, 3), (share, 4), (project, 5)):
            k = i - lag

            @pl.when(jnp.logical_and(k >= 0, k < rounds))
            def _():
                stage(k)

        return carry

    lax.fori_loop(2, rounds + 5, step, 0)
    for k in range(rounds - P_SLOTS, rounds):
        wait_part_sends(k)


def write_out(y_last, v_vm, u_vm, u_hbm, tail, sem):
    tokens, rows = u_vm.shape[0], y_last.shape[0]
    done = pl.ds(0, tokens - rows)
    early = pltpu.make_async_copy(u_vm.at[done], u_hbm.at[done], sem.at[0])
    late = pltpu.make_async_copy(tail, u_hbm.at[pl.ds(tokens - rows, rows)], sem.at[1])
    early.start()
    tail[...] = jnp.dot(y_last[...], v_vm[...], preferred_element_type=jnp.float32).astype(jnp.bfloat16)
    late.start()
    early.wait()
    late.wait()


def solution(mesh):
    ring = mesh.shape["tp"] // 2

    def local_step(x, w, v):
        tokens, depth = x.shape
        width, out = v.shape
        rows = 2 * ring * UNIT
        rounds = tokens // rows
        half = width // 2
        count = len(first_blocks(half))
        dma = pltpu.SemaphoreType.DMA
        f32, bf16 = jnp.float32, jnp.bfloat16
        any_spec = pl.BlockSpec(memory_space=pl.ANY)
        vmem_spec = pl.BlockSpec(memory_space=pltpu.VMEM)
        u, v_kept, y_last = pl.pallas_call(
            functools.partial(reduce_and_project, ring, rounds),
            out_shape=[pltpu.VMEM((tokens, out), bf16), pltpu.VMEM((width, out), bf16), pltpu.VMEM((TAIL * rows, width), bf16)],
            in_specs=[any_spec] * 3,
            out_specs=[vmem_spec] * 3,
            scratch_shapes=[
                pltpu.VMEM((depth, width), bf16),
                pltpu.VMEM((2, rows, depth), bf16),
                pltpu.VMEM((P_SLOTS, 2 * ring, UNIT, width), f32),
                pltpu.VMEM((D_SLOTS, ring, UNIT, width), f32),
                pltpu.VMEM((HOP_SLOTS, 2, UNIT, half), f32),
                pltpu.VMEM((ROOT_SLOTS, 2, 2, UNIT, half), f32),
                pltpu.VMEM((Y_SLOTS, 2 * ring, UNIT, width), bf16),
                dma((count,)), dma, dma((2,)),
                dma((P_SLOTS,)), dma((D_SLOTS, 2)), dma((count,)), dma((count,)), dma((HOP_SLOTS, 2)), dma((ROOT_SLOTS,)),
                dma((Y_SLOTS,)), dma((G_SLOTS, 2, 2)), dma((G_SLOTS,)), dma((Y_SLOTS,)),
            ],
            compiler_params=pltpu.CompilerParams(collective_id=0, has_side_effects=True, vmem_limit_bytes=40_000_000),
            cost_estimate=pl.CostEstimate(flops=2 * tokens * (depth * width + width * out), bytes_accessed=2 * (tokens * depth + depth * width + width * out), transcendentals=0),
        )(x, w, v)
        return pl.pallas_call(
            write_out,
            out_shape=jax.ShapeDtypeStruct((tokens, out), bf16),
            in_specs=[vmem_spec] * 3,
            out_specs=any_spec,
            scratch_shapes=[pltpu.VMEM((TAIL * rows, out), bf16), dma((2,))],
            compiler_params=pltpu.CompilerParams(vmem_limit_bytes=8_000_000),
            cost_estimate=pl.CostEstimate(flops=2 * TAIL * rows * width * out, bytes_accessed=2 * tokens * out, transcendentals=0),
        )(y_last, v_kept, u)

    return jax.shard_map(local_step, mesh=mesh, in_specs=(P("data", "tp"), P("tp", None), P(None, "tp")), out_specs=P("data", "tp"), check_vma=False)
```
